32 devices in a mesh: gx: 8 (over y, x, core), gy: 4 (over z).
Axes of the slice: x: 2, y: 2, z: 4, core: 2. Of those that a mesh axis runs over, the one named last changes fastest.
Arguments:
- queries: bfloat16 [512, 2048], P(('gx', 'gy')), may hold values from -6 to 6
- probe_dev: int32 [512, 16], P(('gx', 'gy')), may hold values from 0 to 31, all different within a row; in each aligned block of 16 rows (0 to 15, 16 to 31, ...) at most 10 rows name the same one
- probe_list: int32 [512, 16], P(('gx', 'gy')), may hold values from 0 to 15
- documents: bfloat16 [512, 256, 2048], P(('gx', 'gy')), may hold values from -6 to 6
- lengths: int32 [512], P(('gx', 'gy')), may hold values from 96 to 256, as said below
- short_dev: int32 [512, 32], P(('gx', 'gy')), may hold values from 0 to 31, all different within a row; in each aligned block of 16 rows (0 to 15, 16 to 31, ...) at most 16 rows name the same one
- short_list: int32 [512, 32], P(('gx', 'gy')), may hold values from 0 to 15
- short_row: int32 [512, 32], P(('gx', 'gy')), may hold values from 0 to 95
Outputs:
- prefix_top: float32 [512, 32], P(('gx', 'gy'))
- rescored: float32 [512, 32], P(('gx', 'gy'))
The draws below stay inside these ranges and needn't reach their ends.
Inputs may be any that keep to these rules, and one draw needn't show every extreme that they name: `lengths`: every list holds at least 96 documents, and in every draw some list is full. `probe_dev`: the 16 entries of a query name different devices. Among the 16 queries of one device, no device is named more than 10 times, and some device is named exactly 10 times. `short_dev`: the 32 entries of a query name different devices. Among the 16 queries of one device, no device is named more than 16 times, and some device is named exactly 16 times.
All inputs are finite; a program needn't handle non-finite values.
Results may differ from the reference program's by a relative error of at most 0.0029.
Values may be sent and summed in bfloat16 or wider, within the bound.
A program may use at most 128 MiB of HBM per device.

```python
import math
import jax
import jax.numpy as jnp
import numpy as np
from jax import lax

QRY_DEV = 16
LISTS_DEV = 16
ROWS = 256
LEN_MIN = 96
PREFIX = 256
FULL = 2048
PROBES = 16
TOPK = 32
SHORT = 32
QUERIES = 512
LISTS = 512
CAP = 16
PCAP = 10
DEVICES = 32


def draw_lengths(key, part):
    first_key, second_key = jax.random.split(jax.random.fold_in(key, 17))
    counts = jax.random.randint(first_key, (LISTS,), LEN_MIN, ROWS + 1)
    full_spot = jax.random.randint(second_key, (), 0, LISTS)
    return jnp.where(jnp.arange(LISTS) == full_spot, ROWS, counts).astype(jnp.int32)


def plant(entries, key, smallest, top_value):
    spot = [jax.random.randint(jax.random.fold_in(key, axis), (), 0, length) for axis, length in enumerate(entries.shape)]
    main_axis = entries.shape.index(max(entries.shape))
    neighbour = spot[:main_axis] + [(spot[main_axis] + 1) % entries.shape[main_axis]] + spot[main_axis + 1:]
    return entries.at[tuple(spot)].set(smallest).at[tuple(neighbour)].set(top_value)


def steps_of(rng, extent, cuts, least, largest):
    factor_of, own = 1.0, jax.random.fold_in(rng, 6)
    for position, blocks in cuts:
        steps = jnp.exp(jax.random.uniform(jax.random.fold_in(own, position), (blocks,), jnp.float32, least / len(cuts), largest / len(cuts)))
        factor_of = factor_of * jnp.repeat(steps, extent[position] // blocks).reshape([-1 if axis == position else 1 for axis in range(len(extent))])
    return factor_of


def deal_out(own_key, own, number, rows, number_of, top, reach, skew):
    ranking = jax.random.permutation(own_key, number_of)
    heavy_load, ordinary = load_shares(number_of, rows * top, reach, skew, True), load_shares(number_of, rows * top, reach, skew, False)
    places = jnp.arange(number_of)

    def named(sizes, offset_by):
        used = int((sizes > 0).sum())
        fixed = max(1, used // 4)
        shifted = fixed + (places - fixed + offset_by * (used - fixed)) % max(1, number_of - fixed)
        return jnp.zeros((number_of,), jnp.int32).at[ranking[jnp.where(places < fixed, places, shifted)]].set(jnp.asarray(sizes, jnp.int32))

    sizes = jnp.where(number % 4 == 0, named(heavy_load, number // 4), named(ordinary, number - number // 4 - 1))
    mixed = jax.random.permutation(jax.random.fold_in(own, 3), number_of)
    giver, taker = mixed[0:number_of // 2 * 2:2], mixed[1:number_of // 2 * 2:2]
    margin = jnp.minimum(sizes[giver] - 1, reach - sizes[taker]) // 2
    margin = jnp.where((giver == ranking[0]) | (taker == ranking[0]) | (sizes[taker] == 0), 0, jnp.maximum(margin, 0))
    shifted = jax.random.randint(jax.random.fold_in(own, 4), (number_of // 2,), 0, 1 << 20) % (margin + 1)
    sizes = sizes.at[giver].add(-shifted).at[taker].add(shifted)
    members = jnp.searchsorted(jnp.cumsum(sizes), jnp.arange(rows * top), side="right").astype(jnp.int32)
    table = members.reshape(top, rows).T
    table = table[jax.random.permutation(jax.random.fold_in(own, 1), rows)]
    offset_by = jax.random.randint(jax.random.fold_in(own, 2), (rows, 1), 0, top)
    return jnp.take_along_axis(table, (jnp.arange(top)[None, :] + offset_by) % top, axis=1)


def load_shares(count, total, reach, skew, full):
    portions = [(1 << 20) // math.isqrt(grade ** skew) + 1 for grade in range(1, count + 1)]
    largest = reach if full else min(reach, max(-(-total // count), total * portions[0] // sum(portions)))
    least = 1 if total - largest >= count - 1 else 0
    given, rest = [largest] + [least] * (count - 1), total - largest - least * (count - 1)
    while rest > 0:
        movable = [i for i in range(1, count) if given[i] < largest] or [i for i in range(1, count) if given[i] < reach]
        whole, budget = sum([portions[i] for i in movable]), rest
        for i in movable:
            extra = min(reach - given[i], max(1, budget * portions[i] // whole), rest)
            given[i] = given[i] + extra
            rest = rest - extra
    return np.array(given)


def gaussian(rng, shape, deviation, bound, cuts=(), held_as=jnp.bfloat16):
    result = jax.random.normal(rng, shape, jnp.float32) * deviation
    if len(cuts) > 0:
        result = steps_of(rng, shape, cuts, -0.22, 0.18) * result
    return jnp.clip(result, min=-bound, max=bound).astype(held_as)


def setup_inputs(seed: int = 0) -> dict:
    key_of = jax.random.split(jax.random.key(seed), 9)
    queries = gaussian(key_of[0], (QUERIES, FULL), 1.0, 6.0, ((0, 32),))
    probe_dev_keys = jax.random.split(jax.random.fold_in(key_of[1], 1), QUERIES // QRY_DEV)
    probe_dev_turns = jax.random.permutation(jax.random.fold_in(key_of[1], 3), QUERIES // QRY_DEV)
    probe_dev = jax.vmap(lambda own, number: deal_out(jax.random.fold_in(key_of[1], 2), own, number, QRY_DEV, DEVICES, PROBES, PCAP, 2))(probe_dev_keys, probe_dev_turns).reshape((QUERIES, PROBES))
    probe_list = plant(jax.random.randint(key_of[2], (QUERIES, PROBES), 0, LISTS_DEV), jax.random.fold_in(key_of[2], 1), 0, LISTS_DEV - 1).astype(jnp.int32)
    documents = gaussian(key_of[3], (LISTS, ROWS, FULL), 1.0, 6.0, ((0, 32),))
    lengths = draw_lengths(jax.random.fold_in(key_of[8], 71), 0)
    short_dev_keys = jax.random.split(jax.random.fold_in(key_of[5], 1), QUERIES // QRY_DEV)
    short_dev_turns = jax.random.permutation(jax.random.fold_in(key_of[5], 3), QUERIES // QRY_DEV)
    short_dev = jax.vmap(lambda own, number: deal_out(jax.random.fold_in(key_of[5], 2), own, number, QRY_DEV, DEVICES, SHORT, CAP, 1))(short_dev_keys, short_dev_turns).reshape((QUERIES, SHORT))
    short_list = plant(jax.random.randint(key_of[6], (QUERIES, SHORT), 0, LISTS_DEV), jax.random.fold_in(key_of[6], 1), 0, LISTS_DEV - 1).astype(jnp.int32)
    short_row = plant(jax.random.randint(key_of[7], (QUERIES, SHORT), 0, LEN_MIN), jax.random.fold_in(key_of[7], 1), 0, LEN_MIN - 1).astype(jnp.int32)
    return dict(queries=queries, probe_dev=probe_dev, probe_list=probe_list, documents=documents, lengths=lengths, short_dev=short_dev, short_list=short_list, short_row=short_row)


def unit_rows(values):
    return values / jnp.sqrt(1.0 + lax.optimization_barrier(jnp.sum(values * values, axis=1, keepdims=True)))

def top_values(values, count):
    return -jnp.sort(-values, axis=-1)[..., :count]

def reference(queries, probe_dev, probe_list, documents, lengths, short_dev, short_list, short_row):
    query_float = queries.astype(jnp.float32)
    prefix_unit = unit_rows(query_float[:, :PREFIX]).astype(jnp.bfloat16)
    full_unit = unit_rows(query_float).astype(jnp.bfloat16)
    doc_prefix = documents[:, :, :PREFIX]
    probes = (probe_dev * LISTS_DEV + probe_list).astype(jnp.int32)
    query_total = queries.shape[0]
    block_rows = 64 if query_total % 64 == 0 else query_total

    def top_block(inputs):
        prefix_block, probe_block = inputs
        gathered = doc_prefix[probe_block]
        scores = jnp.einsum('bd,bprd->bpr', prefix_block.astype(jnp.float32), gathered.astype(jnp.float32))
        valid_rows = jnp.arange(ROWS)[None, None, :] < lengths[probe_block][:, :, None]
        masked = jnp.where(valid_rows, scores, -jnp.inf).reshape(prefix_block.shape[0], -1)
        return top_values(masked, TOPK)
    prefix_top = lax.map(top_block, (prefix_unit.reshape(-1, block_rows, PREFIX), probes.reshape(-1, block_rows, PROBES))).reshape(query_total, TOPK)

    def rescore_block(inputs):
        unit_block, dev_block, list_block, row_block = inputs
        list_index = (dev_block * LISTS_DEV + list_block).astype(jnp.int32)
        vectors = documents[list_index, row_block.astype(jnp.int32)]
        return jnp.einsum('bsf,bf->bs', vectors.astype(jnp.float32), unit_block.astype(jnp.float32))
    rescored = lax.map(rescore_block, (full_unit.reshape(-1, block_rows, FULL), short_dev.reshape(-1, block_rows, SHORT), short_list.reshape(-1, block_rows, SHORT), short_row.reshape(-1, block_rows, SHORT))).reshape(query_total, SHORT)
    return (prefix_top, rescored)
```

```python
import functools

import jax
import jax.numpy as jnp
from jax import lax
from jax.experimental import pallas as pl
from jax.experimental.pallas import tpu as pltpu
from jax.sharding import PartitionSpec as P

PREFIX = 256
TOPK = 32
SHORT_ROWS = 96
AXES = ("gx", "gy")
LANES = 128
HALF = 64
NT = (((1,), (1,)), ((), ()))


def unit_rows(values):
    return values / jnp.sqrt(1.0 + jnp.sum(values * values, axis=1, keepdims=True))


def sort_pairs(n):
    p = 1
    while p < n:
        k = p
        while k >= 1:
            for j in range(k % p, n - k, 2 * k):
                for i in range(min(k, n - j - k)):
                    if (i + j) // (2 * p) == (i + j + k) // (2 * p):
                        yield i + j, i + j + k
            k //= 2
        p *= 2


def sort_desc(v):
    v = list(v)
    for a, b in sort_pairs(len(v)):
        v[a], v[b] = jnp.maximum(v[a], v[b]), jnp.minimum(v[a], v[b])
    return v


def merge_top(a, b):
    n = len(a)
    v = [jnp.maximum(a[i], b[n - 1 - i]) for i in range(n)]
    step = n // 2
    while step:
        for i in range(n):
            if not i & step:
                v[i], v[i + step] = jnp.maximum(v[i], v[i + step]), jnp.minimum(v[i], v[i + step])
        step //= 2
    return v


def score_kernel(probes, shorts, all_ref, len_ref, docs_ref, out_ref, pre_docs, top_docs, chosen, result, sems):
    lists, rows, full = docs_ref.shape
    total = all_ref.shape[0]
    per_dev = 16
    me = (lax.axis_index("gx") * lax.axis_size("gy") + lax.axis_index("gy")).astype(jnp.float32)
    pre_copy = pltpu.make_async_copy(docs_ref.at[:, :, pl.ds(0, PREFIX)], pre_docs, sems.at[0])
    top_copy = pltpu.make_async_copy(docs_ref.at[:, pl.ds(0, SHORT_ROWS), :], top_docs, sems.at[1])
    pre_copy.start()
    top_copy.start()
    pre_copy.wait()
    top_copy.wait()
    tile = chosen.shape[1]
    chunk = 32
    group = 4
    result[...] = jnp.zeros_like(result)

    @pl.loop(0, total // tile)
    def _(block):
        mine = pl.ds(pl.multiple_of(block * tile, tile), tile)
        codes = jnp.transpose(all_ref[mine, full + PREFIX:].astype(jnp.float32))
        p_dev, p_list = codes[:probes], codes[probes:2 * probes]
        base = 2 * probes
        s_dev, s_list, s_row = (codes[base + i * shorts:base + (i + 1) * shorts] for i in range(3))
        probed = jnp.sum(jnp.where(p_dev == me, p_list + 1.0, 0.0), axis=0, keepdims=True).astype(jnp.int32) - 1
        wanted = jnp.sum(jnp.where(s_dev == me, s_list * rows + s_row + 1.0, 0.0), axis=0, keepdims=True).astype(jnp.int32) - 1

        @pl.loop(0, rows // chunk)
        def _(c):
            first = pl.multiple_of(c * chunk, chunk)
            docs = pre_docs[:, pl.ds(first, chunk), :].reshape(lists * chunk, PREFIX)
            scores = lax.dot_general(docs, all_ref[mine, full:full + PREFIX], NT, preferred_element_type=jnp.float32)
            slot = lax.broadcasted_iota(jnp.int32, (chunk, tile), 0) + first
            value = jnp.full((chunk, tile), -jnp.inf, jnp.float32)
            for l in range(lists):
                limit = jnp.where(probed == l, len_ref[l], 0)
                value = jnp.where(slot < limit, scores[l * chunk:(l + 1) * chunk], value)
            chosen[pl.ds(first, chunk), :] = value

        @pl.loop(0, tile // LANES)
        def _(t):
            lanes = pl.ds(pl.multiple_of(t * LANES, LANES), LANES)
            v = [chosen[pl.ds(8 * i, 8), lanes] for i in range(rows // 8)]
            parts = [sort_desc(v[i:i + TOPK]) for i in range(0, len(v), TOPK)]
            v = functools.reduce(merge_top, parts)
            for shift in (4, 2, 1):
                v = merge_top(v, [pltpu.roll(x, shift, 0) for x in v])
            sub = lax.broadcasted_iota(jnp.int32, (8, LANES), 0)
            for a in range(TOPK // 8):
                packed = v[8 * a]
                for s in range(1, 8):
                    packed = jnp.where(sub == s, v[8 * a + s], packed)
                result[pl.ds(8 * a, 8), lanes] = packed

        def rescore(g, acc):
            docs = top_docs[pl.ds(g * group, group)].reshape(group * SHORT_ROWS, full)
            scores = lax.dot_general(docs, all_ref[mine, :full], NT, preferred_element_type=jnp.float32)
            slot = lax.broadcasted_iota(jnp.int32, (SHORT_ROWS, tile), 0)
            for j in range(group):
                hit = slot == wanted - (g * group + j) * rows
                part = jnp.where(hit, scores[j * SHORT_ROWS:(j + 1) * SHORT_ROWS], 0.0)
                acc = acc + jnp.sum(part.reshape(SHORT_ROWS // 8, 8, tile), axis=0)
            return acc

        acc = lax.fori_loop(0, lists // group, rescore, jnp.zeros((8, tile), jnp.float32))
        result[TOPK:TOPK + 8, :] = jnp.broadcast_to(jnp.sum(acc, axis=0, keepdims=True), (8, tile))
        lane = lax.broadcasted_iota(jnp.int32, (8, LANES), 1)
        for t in range(tile // LANES):
            turned = jnp.transpose(result[:, t * LANES:(t + 1) * LANES])
            for d in range(LANES // per_dev):
                low = turned[d * per_dev:d * per_dev + 8]
                high = pltpu.roll(turned[d * per_dev + 8:(d + 1) * per_dev], HALF, 1)
                out_ref[block * (tile // per_dev) + t * (LANES // per_dev) + d] = jnp.where(lane < HALF, low, high)


def merge_kernel(got_ref, dev_ref, top_ref, short_ref):
    count = got_ref.shape[0]
    shorts = dev_ref.shape[1]
    v = [got_ref[i] for i in range(count)]
    pad = -count % TOPK
    v = v + [jnp.full_like(v[0], -jnp.inf)] * pad
    parts = [sort_desc(v[i:i + TOPK]) for i in range(0, len(v), TOPK)]
    best = functools.reduce(merge_top, parts)
    shift = TOPK // 2
    while shift:
        best = merge_top(best, [pltpu.roll(x, LANES - shift, 1) for x in best])
        shift //= 2
    lane = lax.broadcasted_iota(jnp.int32, (8, LANES), 1)
    out = best[0]
    for i in range(1, TOPK):
        out = jnp.where(lane % HALF == i, pltpu.roll(best[i], i, 1), out)
    top_ref[0:8, :] = out[:, :TOPK]
    top_ref[8:16, :] = pltpu.roll(out, HALF, 1)[:, :TOPK]
    for h in range(2):
        dev = dev_ref[8 * h:8 * h + 8, :]
        acc = jnp.zeros((8, shorts), jnp.float32)
        for i in range(count):
            spot = HALF * h + TOPK
            acc = jnp.where(dev == i, jnp.broadcast_to(got_ref[i][:, spot:spot + 1], (8, shorts)), acc)
        short_ref[8 * h:8 * h + 8, :] = acc


def shards(queries, probe_dev, probe_list, documents, lengths, short_dev, short_list, short_row):
    count = lax.axis_size(AXES)
    lists, rows, full = documents.shape
    query_rows = queries.shape[0]
    probes, shorts = probe_dev.shape[1], short_dev.shape[1]
    query_float = queries.astype(jnp.float32)
    codes = jnp.concatenate([probe_dev, probe_list, short_dev, short_list, short_row], axis=1)
    packed = jnp.concatenate([
        unit_rows(query_float).astype(jnp.bfloat16),
        unit_rows(query_float[:, :PREFIX]).astype(jnp.bfloat16),
        codes.astype(jnp.bfloat16),
    ], axis=1)
    everyone = lax.all_gather(packed, AXES, axis=0, tiled=True)
    total = count * query_rows
    tile = min(512, total)
    vmem = pl.BlockSpec(memory_space=pltpu.VMEM)
    returned = pl.pallas_call(
        functools.partial(score_kernel, probes, shorts),
        out_shape=jax.ShapeDtypeStruct((count, 8, LANES), jnp.float32),
        in_specs=[vmem, pl.BlockSpec(memory_space=pltpu.SMEM), pl.BlockSpec(memory_space=pl.ANY)],
        out_specs=vmem,
        scratch_shapes=[
            pltpu.VMEM((lists, rows, PREFIX), jnp.bfloat16),
            pltpu.VMEM((lists, SHORT_ROWS, full), jnp.bfloat16),
            pltpu.VMEM((rows, tile), jnp.float32),
            pltpu.VMEM((LANES, tile), jnp.float32),
            pltpu.SemaphoreType.DMA((2,)),
        ],
        compiler_params=pltpu.CompilerParams(vmem_limit_bytes=60 * 1024 * 1024),
        name="score",
    )(everyone, lengths, documents)
    got = lax.all_to_all(returned, AXES, split_axis=0, concat_axis=0, tiled=True)
    return pl.pallas_call(
        merge_kernel,
        out_shape=(
            jax.ShapeDtypeStruct((query_rows, TOPK), jnp.float32),
            jax.ShapeDtypeStruct((query_rows, shorts), jnp.float32),
        ),
        in_specs=[vmem, vmem],
        out_specs=(vmem, vmem),
        name="merge",
    )(got, short_dev)


def solution(mesh):
    one = P(AXES, None)
    in_specs = (one, one, one, P(AXES, None, None), P(AXES), one, one, one)
    return jax.shard_map(shards, mesh=mesh, in_specs=in_specs, out_specs=(one, one), check_vma=False)
```

```python
import functools

import jax
import jax.numpy as jnp
from jax import lax
from jax.experimental import pallas as pl
from jax.experimental.pallas import tpu as pltpu
from jax.sharding import PartitionSpec as P

PREFIX = 256
TOPK = 32
SHORT_ROWS = 96
AXES = ("gx", "gy")
LANES = 128
HALF = 64
NT = (((1,), (1,)), ((), ()))
MESH = pl.DeviceIdType.MESH


def unit_rows(values):
    return values / jnp.sqrt(1.0 + jnp.sum(values * values, axis=1, keepdims=True))


def sort_pairs(n):
    p = 1
    while p < n:
        k = p
        while k >= 1:
            for j in range(k % p, n - k, 2 * k):
                for i in range(min(k, n - j - k)):
                    if (i + j) // (2 * p) == (i + j + k) // (2 * p):
                        yield i + j, i + j + k
            k //= 2
        p *= 2


def sort_desc(v):
    v = list(v)
    for a, b in sort_pairs(len(v)):
        v[a], v[b] = jnp.maximum(v[a], v[b]), jnp.minimum(v[a], v[b])
    return v


def merge_top(a, b):
    n = len(a)
    v = [jnp.maximum(a[i], b[n - 1 - i]) for i in range(n)]
    step = n // 2
    while step:
        for i in range(n):
            if not i & step:
                v[i], v[i + step] = jnp.maximum(v[i], v[i + step]), jnp.minimum(v[i], v[i + step])
        step //= 2
    return v


def device_of(position):
    size = lax.axis_size("gy")
    return position // size, position % size


def gather_kernel(split, q_ref, code_ref, a_ref, b_ref, line_send, line_recv, cube_send, cube_recv):
    gx, gy = lax.axis_index("gx"), lax.axis_index("gy")
    line = lax.axis_size("gy")
    bits = len(a_ref.shape) - 3
    outs = (a_ref, b_ref)

    def flip(bit):
        size = 1 << bit
        return gx + (1 - 2 * ((gx // size) % 2)) * size

    def view(ref, free, slot):
        spots = [slice(None) if b in free else (gx // (1 << b)) % 2 for b in range(bits - 1, -1, -1)]
        return ref.at[tuple(spots) + (slot,)]

    barrier = pltpu.get_barrier_semaphore()
    for k in range(1, line):
        pl.semaphore_signal(barrier, inc=1, device_id=(gx, (gy + k) % line), device_id_type=MESH)
    for b in range(bits):
        pl.semaphore_signal(barrier, inc=1, device_id=(flip(b), gy), device_id_type=MESH)
    values = q_ref[...].astype(jnp.float32)
    unit = unit_rows(values).astype(jnp.bfloat16)
    view(a_ref, (), gy)[...] = unit[:, :split]
    rest = unit.shape[1] - split
    own = view(b_ref, (), gy)
    own[:, :rest] = unit[:, split:]
    own[:, rest:rest + PREFIX] = unit_rows(values[:, :PREFIX]).astype(jnp.bfloat16)
    own[:, rest + PREFIX:] = code_ref[...]
    pl.semaphore_wait(barrier, line - 1 + bits)

    offsets = sorted(range(1, line), key=lambda k: (min(k, line - k), k))

    def line_copy(piece, k):
        ref = outs[piece]
        return pltpu.make_async_remote_copy(
            src_ref=view(ref, (), gy), dst_ref=view(ref, (), gy),
            send_sem=line_send.at[piece, k], recv_sem=line_recv.at[piece, k],
            device_id=(gx, (gy + k) % line), device_id_type=MESH,
        )

    order = (list(range(1, bits)) + [0], list(range(bits - 1, 0, -1)) + [0])

    def cube_copy(piece, k, step):
        ref, slot = outs[piece], (gy + line - k) % line
        src = view(ref, order[piece][:step], slot)
        return pltpu.make_async_remote_copy(
            src_ref=src, dst_ref=src,
            send_sem=cube_send.at[piece, k, step], recv_sem=cube_recv.at[piece, k, step],
            device_id=(flip(order[piece][step]), gy), device_id_type=MESH,
        )

    steps = bits
    slots = [0] + offsets
    for k in offsets:
        for piece in range(2):
            line_copy(piece, k).start()
    for wave in range(len(slots) + steps):
        for step in range(steps, -1, -1):
            if not 0 <= wave - step < len(slots):
                continue
            k = slots[wave - step]
            for piece in range(2):
                if step == 0 and k:
                    line_copy(piece, k).wait_recv()
                if step > 0:
                    cube_copy(piece, k, step - 1).wait_recv()
                if step < steps:
                    cube_copy(piece, k, step).start()
    for piece in range(2):
        for k in offsets:
            line_copy(piece, k).wait_send()
        for k in slots:
            for step in range(steps):
                cube_copy(piece, k, step).wait_send()


def exchange_kernel(src_ref, out_ref, send_sem, recv_sem, own_sem):
    count = src_ref.shape[0]
    me = lax.axis_index("gx") * lax.axis_size("gy") + lax.axis_index("gy")
    barrier = pltpu.get_barrier_semaphore()

    @pl.loop(1, count)
    def _(k):
        pl.semaphore_signal(barrier, inc=1, device_id=device_of((me + k) % count), device_id_type=MESH)

    own = pltpu.make_async_copy(src_ref.at[me], out_ref.at[me], own_sem)
    own.start()
    pl.semaphore_wait(barrier, count - 1)

    def copy(k):
        peer = (me + k) % count
        return pltpu.make_async_remote_copy(
            src_ref=src_ref.at[peer], dst_ref=out_ref.at[me],
            send_sem=send_sem.at[k], recv_sem=recv_sem.at[k],
            device_id=device_of(peer), device_id_type=MESH,
        )

    @pl.loop(1, count)
    def _(k):
        copy(k).start()

    own.wait()

    @pl.loop(1, count)
    def _(k):
        copy(k).wait_recv()

    @pl.loop(1, count)
    def _(k):
        copy(k).wait_send()


def score_kernel(probes, shorts, a_ref, b_ref, len_ref, docs_ref, out_ref, pre_docs, top_docs, chosen, result, sems):
    lists, rows, full = docs_ref.shape
    total, split = a_ref.shape
    rest = full - split
    per_dev = 16
    me = (lax.axis_index("gx") * lax.axis_size("gy") + lax.axis_index("gy")).astype(jnp.float32)
    pre_copy = pltpu.make_async_copy(docs_ref.at[:, :, pl.ds(0, PREFIX)], pre_docs, sems.at[0])
    top_copy = pltpu.make_async_copy(docs_ref.at[:, pl.ds(0, SHORT_ROWS), :], top_docs, sems.at[1])
    pre_copy.start()
    top_copy.start()
    pre_copy.wait()
    top_copy.wait()
    tile = chosen.shape[1]
    chunk = 32
    group = 4
    result[...] = jnp.zeros_like(result)

    @pl.loop(0, total // tile)
    def _(block):
        mine = pl.ds(pl.multiple_of(block * tile, tile), tile)
        codes = jnp.transpose(b_ref[mine, rest + PREFIX:].astype(jnp.float32))
        p_dev, p_list = codes[:probes], codes[probes:2 * probes]
        base = 2 * probes
        s_dev, s_list, s_row = (codes[base + i * shorts:base + (i + 1) * shorts] for i in range(3))
        probed = jnp.sum(jnp.where(p_dev == me, p_list + 1.0, 0.0), axis=0, keepdims=True).astype(jnp.int32) - 1
        wanted = jnp.sum(jnp.where(s_dev == me, s_list * rows + s_row + 1.0, 0.0), axis=0, keepdims=True).astype(jnp.int32) - 1

        @pl.loop(0, rows // chunk)
        def _(c):
            first = pl.multiple_of(c * chunk, chunk)
            docs = pre_docs[:, pl.ds(first, chunk), :].reshape(lists * chunk, PREFIX)
            scores = lax.dot_general(docs, b_ref[mine, rest:rest + PREFIX], NT, preferred_element_type=jnp.float32)
            slot = lax.broadcasted_iota(jnp.int32, (chunk, tile), 0) + first
            value = jnp.full((chunk, tile), -jnp.inf, jnp.float32)
            for l in range(lists):
                limit = jnp.where(probed == l, len_ref[l], 0)
                value = jnp.where(slot < limit, scores[l * chunk:(l + 1) * chunk], value)
            chosen[pl.ds(first, chunk), :] = value

        @pl.loop(0, tile // LANES)
        def _(t):
            lanes = pl.ds(pl.multiple_of(t * LANES, LANES), LANES)
            v = [chosen[pl.ds(8 * i, 8), lanes] for i in range(rows // 8)]
            parts = [sort_desc(v[i:i + TOPK]) for i in range(0, len(v), TOPK)]
            v = functools.reduce(merge_top, parts)
            for shift in (4, 2, 1):
                v = merge_top(v, [pltpu.roll(x, shift, 0) for x in v])
            sub = lax.broadcasted_iota(jnp.int32, (8, LANES), 0)
            for a in range(TOPK // 8):
                packed = v[8 * a]
                for s in range(1, 8):
                    packed = jnp.where(sub == s, v[8 * a + s], packed)
                result[pl.ds(8 * a, 8), lanes] = packed

        def rescore(g, acc):
            docs = top_docs[pl.ds(g * group, group)].reshape(group * SHORT_ROWS, full)
            scores = lax.dot_general(docs[:, :split], a_ref[mine, :], NT, preferred_element_type=jnp.float32)
            scores = scores + lax.dot_general(docs[:, split:], b_ref[mine, :rest], NT, preferred_element_type=jnp.float32)
            slot = lax.broadcasted_iota(jnp.int32, (SHORT_ROWS, tile), 0)
            for j in range(group):
                hit = slot == wanted - (g * group + j) * rows
                part = jnp.where(hit, scores[j * SHORT_ROWS:(j + 1) * SHORT_ROWS], 0.0)
                acc = acc + jnp.sum(part.reshape(SHORT_ROWS // 8, 8, tile), axis=0)
            return acc

        acc = lax.fori_loop(0, lists // group, rescore, jnp.zeros((8, tile), jnp.float32))
        result[TOPK:TOPK + 8, :] = jnp.broadcast_to(jnp.sum(acc, axis=0, keepdims=True), (8, tile))
        lane = lax.broadcasted_iota(jnp.int32, (8, LANES), 1)
        for t in range(tile // LANES):
            turned = jnp.transpose(result[:, t * LANES:(t + 1) * LANES])
            for d in range(LANES // per_dev):
                low = turned[d * per_dev:d * per_dev + 8]
                high = pltpu.roll(turned[d * per_dev + 8:(d + 1) * per_dev], HALF, 1)
                out_ref[block * (tile // per_dev) + t * (LANES // per_dev) + d] = jnp.where(lane < HALF, low, high)


def merge_kernel(got_ref, dev_ref, top_ref, short_ref):
    count = got_ref.shape[0]
    shorts = dev_ref.shape[1]
    v = [got_ref[i] for i in range(count)]
    pad = -count % TOPK
    v = v + [jnp.full_like(v[0], -jnp.inf)] * pad
    parts = [sort_desc(v[i:i + TOPK]) for i in range(0, len(v), TOPK)]
    best = functools.reduce(merge_top, parts)
    shift = TOPK // 2
    while shift:
        best = merge_top(best, [pltpu.roll(x, LANES - shift, 1) for x in best])
        shift //= 2
    lane = lax.broadcasted_iota(jnp.int32, (8, LANES), 1)
    out = best[0]
    for i in range(1, TOPK):
        out = jnp.where(lane % HALF == i, pltpu.roll(best[i], i, 1), out)
    top_ref[0:8, :] = out[:, :TOPK]
    top_ref[8:16, :] = pltpu.roll(out, HALF, 1)[:, :TOPK]
    for h in range(2):
        dev = dev_ref[8 * h:8 * h + 8, :]
        acc = jnp.zeros((8, shorts), jnp.float32)
        for i in range(count):
            spot = HALF * h + TOPK
            acc = jnp.where(dev == i, jnp.broadcast_to(got_ref[i][:, spot:spot + 1], (8, shorts)), acc)
        short_ref[8 * h:8 * h + 8, :] = acc


def shards(queries, probe_dev, probe_list, documents, lengths, short_dev, short_list, short_row):
    count = lax.axis_size(AXES)
    lists, rows, full = documents.shape
    query_rows = queries.shape[0]
    probes, shorts = probe_dev.shape[1], short_dev.shape[1]
    codes = jnp.concatenate([probe_dev, probe_list, short_dev, short_list, short_row], axis=1)
    line = lax.axis_size("gy")
    bits = (count // line).bit_length() - 1
    split = (full + PREFIX + LANES + 2 * LANES - 1) // (2 * LANES) * LANES
    widths = (split, full - split + PREFIX + codes.shape[1])
    vmem = pl.BlockSpec(memory_space=pltpu.VMEM)
    everyone = pl.pallas_call(
        functools.partial(gather_kernel, split),
        out_shape=tuple(
            jax.ShapeDtypeStruct((2,) * bits + (line, query_rows, width), jnp.bfloat16) for width in widths
        ),
        in_specs=[vmem, vmem],
        out_specs=(vmem, vmem),
        scratch_shapes=[
            pltpu.SemaphoreType.DMA((2, line)),
            pltpu.SemaphoreType.DMA((2, line)),
            pltpu.SemaphoreType.DMA((2, line, bits)),
            pltpu.SemaphoreType.DMA((2, line, bits)),
        ],
        compiler_params=pltpu.CompilerParams(collective_id=0, has_side_effects=True),
        name="gather",
    )(queries, codes.astype(jnp.bfloat16))
    everyone = [x.reshape(-1, x.shape[-1]) for x in everyone]
    total = count * query_rows
    tile = min(512, total)
    returned = pl.pallas_call(
        functools.partial(score_kernel, probes, shorts),
        out_shape=jax.ShapeDtypeStruct((count, 8, LANES), jnp.float32),
        in_specs=[vmem, vmem, pl.BlockSpec(memory_space=pltpu.SMEM), pl.BlockSpec(memory_space=pl.ANY)],
        out_specs=vmem,
        scratch_shapes=[
            pltpu.VMEM((lists, rows, PREFIX), jnp.bfloat16),
            pltpu.VMEM((lists, SHORT_ROWS, full), jnp.bfloat16),
            pltpu.VMEM((rows, tile), jnp.float32),
            pltpu.VMEM((LANES, tile), jnp.float32),
            pltpu.SemaphoreType.DMA((2,)),
        ],
        compiler_params=pltpu.CompilerParams(vmem_limit_bytes=60 * 1024 * 1024),
        name="score",
    )(*everyone, lengths, documents)
    got = pl.pallas_call(
        exchange_kernel,
        out_shape=jax.ShapeDtypeStruct(returned.shape, returned.dtype),
        in_specs=[vmem],
        out_specs=vmem,
        scratch_shapes=[
            pltpu.SemaphoreType.DMA((count,)),
            pltpu.SemaphoreType.DMA((count,)),
            pltpu.SemaphoreType.DMA,
        ],
        compiler_params=pltpu.CompilerParams(collective_id=1, has_side_effects=True),
        name="exchange",
    )(returned)
    return pl.pallas_call(
        merge_kernel,
        out_shape=(
            jax.ShapeDtypeStruct((query_rows, TOPK), jnp.float32),
            jax.ShapeDtypeStruct((query_rows, shorts), jnp.float32),
        ),
        in_specs=[vmem, vmem],
        out_specs=(vmem, vmem),
        name="merge",
    )(got, short_dev)


def solution(mesh):
    one = P(AXES, None)
    in_specs = (one, one, one, P(AXES, None, None), P(AXES), one, one, one)
    return jax.shard_map(shards, mesh=mesh, in_specs=in_specs, out_specs=(one, one), check_vma=False)
```
